256 devices in a mesh: seq: 32 (over z, x_lo, core), fsdp: 8 (over x_hi, y).
Axes of the slice: x: 4 (x_hi: 2, x_lo: 2; x = x_hi * 2 + x_lo), y: 4, z: 8, core: 2. Of those that a mesh axis runs over, the one named last changes fastest.
Arguments:
- hidden_next: bfloat16 [8192, 8192], P('seq'), may hold values from -6 to 6
- values_next: bfloat16 [8192, 8192], P('seq', 'fsdp'), may hold values from -6 to 6
- seg_next: int32 [4], replicated, may hold values from 1 to 4096, 8192 in all
- proj_bc: bfloat16 [8192, 1024], P(('seq', 'fsdp')), may hold values from -0.09375 to 0.09375
- proj_dt: bfloat16 [8192, 128], P(('seq', 'fsdp')), may hold values from -0.0625 to 0.0625
- dt_bias: float32 [128], replicated, may hold values from -4 to -2.5
- decay_rate: float32 [128], replicated, may hold values from 0 to 1, as said below
- skip_gain: float32 [128], replicated, may hold values from 0.5 to 1.5
- bc_prev: bfloat16 [8192, 1024], P('seq'), may hold values from -4 to 4
- dt_prev: float32 [8192, 128], P('seq', 'fsdp'), may hold values from 0.01 to 0.3
- seg_prev: int32 [4], replicated, may hold values from 1 to 4096, 8192 in all
- grad_prev: bfloat16 [8192, 8192], P('seq', 'fsdp'), may hold values from -6 to 6
Outputs:
- out_next: bfloat16 [8192, 8192], P('seq', 'fsdp')
- grad_values: bfloat16 [8192, 8192], P('seq', 'fsdp')
The draws below stay inside these ranges and needn't reach their ends.
Inputs may be any that keep to these rules, and one draw needn't show every extreme that they name: `seg_next`: lengths of the rollout's 4 segments in order, summing to 8192. `seg_prev`: lengths of the rollout's 4 segments in order, summing to 8192. `decay_rate`: positive.
All inputs are finite; a program needn't handle non-finite values.
Results may differ from the reference program's by a relative error of at most 0.0064.
Values may be sent and summed in bfloat16 or wider, within the bound.
A program may use at most 128 MiB of HBM per device.

```python
import math
import jax
import jax.numpy as jnp
import numpy as np
from jax import lax

D = 8192
HW = 128
P_SIZE = 64
GW = 4
N = 128
SPAN = 128
NSEG = 4
SEQ_LEN = 8192
BCW = 1024


def draw_decay_rate(key, part):
    streams = jax.random.split(jax.random.fold_in(key, 11), 3)
    lasting = jax.random.uniform(streams[0], (HW,)) < 0.5
    slow_rate = jnp.exp(jax.random.uniform(streams[1], (HW,), minval=jnp.log(5.0), maxval=jnp.log(20.0))) / SEQ_LEN
    fast_rate = jnp.exp(jax.random.uniform(streams[2], (HW,), minval=jnp.log(0.25), maxval=jnp.log(0.8)))
    return jnp.where(lasting, slow_rate, fast_rate).astype(jnp.float32)


def spiked(values, stream_key, source, target, blocks, factor):
    owner, partner = [(jnp.arange(values.shape[position]) // (values.shape[position] // blocks)).reshape([-1 if axis == position else 1 for axis in range(values.ndim)]) for position in (source, target)]
    chosen = jax.random.permutation(stream_key, blocks)[partner]
    strong = (owner == chosen) | (owner == (partner + blocks // 2) % blocks)
    return jnp.where(strong, factor * values, values)


def block_scale(rng, shape, cuts, least, largest):
    def one(axis_at, shards_of):
        heights = jax.random.uniform(jax.random.fold_in(jax.random.fold_in(rng, 6), axis_at), (shards_of,), jnp.float32, least / len(cuts), largest / len(cuts))
        return jnp.repeat(jnp.exp(heights), shape[axis_at] // shards_of).reshape((-1,) + (1,) * (len(shape) - axis_at - 1))

    factor_of = one(*cuts[0])
    for cut in cuts[1:]:
        factor_of = factor_of * one(*cut)
    return factor_of


def split_up(amount, total, reach, lean):
    loads = [(1 << 20) // math.isqrt(rank ** lean) + 1 for rank in range(2, amount + 1)]
    rest, counts = total - reach - (amount - 1), [1] * (amount - 1)
    while rest > 0:
        free = [i for i in range(amount - 1) if counts[i] < reach]
        pool, left = sum([loads[i] for i in free]), rest
        for i in free:
            extra = min(reach - counts[i], max(1, left * loads[i] // pool), rest)
            counts[i] = counts[i] + extra
            rest = rest - extra
    return np.array([reach] + counts)


def uneven(stream_key, count, total, limit, slope):
    if count == 2:
        one = jax.random.randint(stream_key, (), max(1, total - limit), min(limit, total - 1) + 1)
        return jnp.stack([one, total - one])
    sizes = jnp.asarray(split_up(count, total, limit, slope), jnp.int32)
    pairs = (count - 1) // 2
    donor, sink = sizes[1:1 + 2 * pairs:2], sizes[2:2 + 2 * pairs:2]
    slack = jnp.minimum(donor - 1, limit - sink)
    shifted = jax.random.randint(jax.random.fold_in(stream_key, 1), (pairs,), 0, 1 << 20) % (slack + 1)
    sizes = sizes.at[1:1 + 2 * pairs:2].set(donor - shifted).at[2:2 + 2 * pairs:2].set(sink + shifted)
    return sizes[jax.random.permutation(jax.random.fold_in(stream_key, 2), count)]


def noise(own_key, shape, scale, most, pieces=(), kind=jnp.bfloat16):
    factor_of = block_scale(own_key, shape, pieces, -0.22, 0.18) if pieces else 1.0
    drawn = jax.random.normal(own_key, shape, jnp.float32) * scale * factor_of
    return jnp.minimum(jnp.maximum(drawn, -most), most).astype(kind)


def bell_draw_with(stream_key, extent, width, most, cuts, heavy, held_as=jnp.bfloat16):
    entries = width * jax.random.normal(stream_key, extent, jnp.float32)
    if cuts:
        entries = entries * block_scale(stream_key, extent, cuts, -0.22, 0.18)
    return jnp.clip(spiked(entries, jax.random.fold_in(stream_key, 3), *heavy), -most, most).astype(held_as)


def setup_inputs(seed: int = 0) -> dict:
    splits = jax.random.split(jax.random.key(seed), 13)
    hidden_next = noise(splits[0], (SEQ_LEN, D), 1.0, 6.0, ((0, 32),))
    values_next = noise(splits[1], (SEQ_LEN, HW * P_SIZE), 1.0, 6.0, ((0, 32), (1, 8)))
    seg_next = uneven(splits[2], NSEG, SEQ_LEN, SEQ_LEN // 2, 2).astype(jnp.int32)
    proj_bc = bell_draw_with(splits[3], (D, BCW), (D * 8) ** -0.5, 0.09375, ((0, 256),), (0, 1, 256, 6.0))
    proj_dt = noise(splits[4], (D, HW), D ** -0.5, 0.0625, ((0, 256),))
    dt_bias = jnp.clip(jax.random.uniform(splits[5], (HW,), jnp.float32, -4.0, -2.5), -4.0, -2.5)
    decay_rate = draw_decay_rate(jax.random.fold_in(splits[12], 71), 0)
    skip_gain = jnp.clip(jax.random.uniform(splits[7], (HW,), jnp.float32, 0.5, 1.5), 0.5, 1.5)
    bc_prev = noise(splits[8], (SEQ_LEN, BCW), 0.3, 4.0, ((0, 32),))
    dt_prev = jnp.clip(jnp.exp(math.log(0.3) - 3.4011974 * jax.random.uniform(splits[9], (SEQ_LEN, HW), jnp.float32) ** block_scale(splits[9], (SEQ_LEN, HW), ((0, 32), (1, 8)), -0.2, 0.2)), 0.01, 0.3)
    seg_prev = uneven(splits[10], NSEG, SEQ_LEN, SEQ_LEN // 2, 2).astype(jnp.int32)
    grad_prev = noise(splits[11], (SEQ_LEN, HW * P_SIZE), 1.0, 6.0, ((0, 32), (1, 8)))
    return dict(hidden_next=hidden_next, values_next=values_next, seg_next=seg_next, proj_bc=proj_bc, proj_dt=proj_dt, dt_bias=dt_bias, decay_rate=decay_rate, skip_gain=skip_gain, bc_prev=bc_prev, dt_prev=dt_prev, seg_prev=seg_prev, grad_prev=grad_prev)


def segment_table(lengths, tokens_total):
    bounds = jnp.cumsum(lengths)[:-1].astype(jnp.int32)
    places = jnp.arange(tokens_total + 1, dtype=jnp.int32) - 1
    return jnp.sum((bounds[None, :] <= places[:, None]).astype(jnp.int32), axis=1)


def block_parts(bc_block, dt_block, seg_ext, decay_rate):
    span_len = bc_block.shape[0]
    half_cols = bc_block.shape[1] // 2
    b_vectors = bc_block[:, :half_cols].reshape(span_len, GW, N)
    c_vectors = bc_block[:, half_cols:].reshape(span_len, GW, N)
    before = seg_ext[0]
    segment = seg_ext[1:]
    cumulative = jnp.cumsum(-dt_block * decay_rate[None, :], axis=0)
    final_cum = cumulative[-1]
    places = jnp.arange(span_len)
    linked = (segment[:, None] == segment[None, :]) & (places[:, None] >= places[None, :])
    scores = jnp.einsum("tgn,sgn->gts", c_vectors.astype(jnp.float32), b_vectors.astype(jnp.float32),
                        precision=lax.Precision.HIGHEST)
    by_head = cumulative.T
    spread = by_head[:, :, None] - by_head[:, None, :]
    decays = jnp.exp(jnp.where(linked[None], spread, -jnp.inf))
    weighted = (decays * dt_block.T[:, None, :]).reshape(GW, HW // GW, span_len, span_len)
    mixing = (weighted * scores[:, None]).reshape(HW, span_len, span_len).astype(jnp.bfloat16)
    keep_final = (segment == segment[-1]).astype(jnp.float32)
    linked_in = (segment == before).astype(jnp.float32)
    send_factor = keep_final[:, None] * jnp.exp(final_cum[None, :] - cumulative) * dt_block
    read_factor = linked_in[:, None] * jnp.exp(cumulative)
    carry_decay = (segment[-1] == before).astype(jnp.float32) * jnp.exp(final_cum)
    return b_vectors, c_vectors, mixing, send_factor, read_factor, carry_decay


def outer_sum(values, vectors):
    span_len, heads_all, head_dim = values.shape
    grouped = values.reshape(span_len, GW, heads_all // GW, head_dim).astype(jnp.float32)
    result = jnp.einsum("sgqp,sgn->gqpn", grouped, vectors.astype(jnp.float32), precision=lax.Precision.HIGHEST)
    return result.reshape(heads_all, head_dim, vectors.shape[2])


def read_state(state_now, vectors, factor):
    heads_all, head_dim, state_dim = state_now.shape
    grouped = state_now.reshape(GW, heads_all // GW, head_dim, state_dim)
    result = jnp.einsum("gqpn,tgn->tgqp", grouped, vectors.astype(jnp.float32), precision=lax.Precision.HIGHEST)
    return result.reshape(vectors.shape[0], heads_all, head_dim) * factor[:, :, None]


def forward_rollout(hidden, inputs, lengths, proj_bc, proj_dt, dt_bias, decay_rate, skip_gain):
    dt_all = jax.nn.softplus(jnp.dot(hidden, proj_dt, preferred_element_type=jnp.float32) + dt_bias[None, :])
    bc_all = jnp.dot(hidden, proj_bc, preferred_element_type=jnp.float32).astype(jnp.bfloat16)
    seg_all = segment_table(lengths, SEQ_LEN)

    def advance(state_now, block_id):
        offset = (block_id * SPAN).astype(jnp.int32)
        bc_block = lax.dynamic_slice_in_dim(bc_all, offset, SPAN, 0)
        dt_block = lax.dynamic_slice_in_dim(dt_all, offset, SPAN, 0)
        seg_ext = lax.dynamic_slice_in_dim(seg_all, offset, SPAN + 1, 0)
        values = lax.dynamic_slice_in_dim(inputs, offset, SPAN, 0).reshape(SPAN, HW, P_SIZE)
        b_vectors, c_vectors, mixing, send_factor, read_factor, carry_decay = block_parts(
            bc_block, dt_block, seg_ext, decay_rate)
        inside = jnp.einsum("hts,shp->thp", mixing.astype(jnp.float32), values.astype(jnp.float32),
                            precision=lax.Precision.HIGHEST)
        output = inside + read_state(state_now, c_vectors, read_factor) + skip_gain[None, :, None] * values.astype(jnp.float32)
        scaled = (values.astype(jnp.float32) * send_factor[:, :, None]).astype(jnp.bfloat16)
        state_next = carry_decay[:, None, None] * state_now + outer_sum(scaled, b_vectors)
        return state_next, output.astype(jnp.bfloat16).reshape(SPAN, HW * P_SIZE)

    blocks_all = jnp.arange(SEQ_LEN // SPAN, dtype=jnp.int32)
    _, outputs = lax.scan(advance, jnp.zeros((HW, P_SIZE, N), jnp.float32), blocks_all)
    return outputs.reshape(SEQ_LEN, HW * P_SIZE)


def backward_rollout(bc_all, dt_all, lengths, grads_all, decay_rate, skip_gain):
    seg_all = segment_table(lengths, SEQ_LEN)

    def retreat(state_now, block_id):
        offset = (block_id * SPAN).astype(jnp.int32)
        bc_block = lax.dynamic_slice_in_dim(bc_all, offset, SPAN, 0)
        dt_block = lax.dynamic_slice_in_dim(dt_all, offset, SPAN, 0)
        seg_ext = lax.dynamic_slice_in_dim(seg_all, offset, SPAN + 1, 0)
        grad_block = lax.dynamic_slice_in_dim(grads_all, offset, SPAN, 0).reshape(SPAN, HW, P_SIZE)
        b_vectors, c_vectors, mixing, send_factor, read_factor, carry_decay = block_parts(
            bc_block, dt_block, seg_ext, decay_rate)
        inside = jnp.einsum("hts,thp->shp", mixing.astype(jnp.float32), grad_block.astype(jnp.float32),
                            precision=lax.Precision.HIGHEST)
        output = inside + read_state(state_now, b_vectors, send_factor) + skip_gain[None, :, None] * grad_block.astype(jnp.float32)
        scaled = (grad_block.astype(jnp.float32) * read_factor[:, :, None]).astype(jnp.bfloat16)
        state_next = carry_decay[:, None, None] * state_now + outer_sum(scaled, c_vectors)
        return state_next, output.astype(jnp.bfloat16).reshape(SPAN, HW * P_SIZE)

    blocks_all = jnp.arange(SEQ_LEN // SPAN, dtype=jnp.int32)
    _, outputs = lax.scan(retreat, jnp.zeros((HW, P_SIZE, N), jnp.float32), blocks_all, reverse=True)
    return outputs.reshape(SEQ_LEN, HW * P_SIZE)


def reference(hidden_next, values_next, seg_next, proj_bc, proj_dt, dt_bias, decay_rate, skip_gain,
              bc_prev, dt_prev, seg_prev, grad_prev):
    out_next = forward_rollout(hidden_next, values_next, seg_next, proj_bc, proj_dt, dt_bias, decay_rate, skip_gain)
    grad_values = backward_rollout(bc_prev, dt_prev, seg_prev, grad_prev, decay_rate, skip_gain)
    return out_next, grad_values
```

```python
import functools

import jax
import jax.numpy as jnp
from jax import lax
from jax.experimental import pallas as pl
from jax.experimental.pallas import tpu as pltpu
from jax.sharding import PartitionSpec as P

GW = 4
SPAN = 128
LANES = 128
MESH = pl.DeviceIdType.MESH


def scan_kernel(
    back, count, nblocks, heads, groups, head_dim,
    len_ref, x_ref, p_ref, q_ref, dt_ref, decay_ref, skip_ref,
    out_ref,
    cum_s, cum_t, dt_t, fin_s, fout_s, fexp, inside, pre, keep,
    give, got, got_keep, back_out, back_in,
    give_sem, got_sem, keep_send, keep_recv, out_sem, in_sem,
):
    me = lax.axis_index("seq")
    npair = heads * head_dim // LANES
    per = LANES // head_dim
    pair_group = npair // groups
    share = npair * LANES // count
    slices = LANES // share

    barrier = pltpu.get_barrier_semaphore()

    def greet(k, _):
        peer = lax.rem(me + k, count)
        pl.semaphore_signal(barrier, inc=1, device_id={"seq": peer}, device_id_type=MESH)
        return 0

    lax.fori_loop(1, count, greet, 0)

    bound = []
    total = jnp.int32(0)
    for k in range(3):
        total = total + len_ref[k]
        bound.append(total)

    def seg_of(pos):
        s = jnp.zeros_like(pos)
        for b in bound:
            s = s + (b <= pos).astype(jnp.int32)
        return s

    slab = me * (nblocks * SPAN)
    dim0 = lax.broadcasted_iota(jnp.int32, (SPAN, SPAN), 0)
    dim1 = lax.broadcasted_iota(jnp.int32, (SPAN, SPAN), 1)
    lane = lax.broadcasted_iota(jnp.int32, (1, LANES), 1)
    tril = (dim0 >= dim1).astype(jnp.float32)

    def widen(a, c):
        res = a[:, c * per:c * per + 1]
        for k in range(1, per):
            res = jnp.where(lane >= k * head_dim, a[:, c * per + k:c * per + k + 1], res)
        return jnp.broadcast_to(res, (a.shape[0], LANES))

    for c in range(npair):
        pre[0, c] = jnp.zeros((LANES, LANES), jnp.float32)
        keep[0, c] = jnp.ones((1, LANES), jnp.float32)

    for step in range(nblocks):
        b = nblocks - 1 - step if back else step
        rows = slice(b * SPAN, (b + 1) * SPAN)
        dt = dt_ref[rows, :]
        cum = jnp.dot(tril, -(dt * decay_ref[...]), precision=lax.Precision.HIGHEST,
                      preferred_element_type=jnp.float32)
        end = cum[SPAN - 1:SPAN, :]
        cum_s[rows, :] = cum
        cum_t[b] = cum.T
        dt_t[b] = dt.T
        pos = slab + b * SPAN + lax.broadcasted_iota(jnp.int32, (SPAN, heads), 0)
        seg = seg_of(pos)
        edge = slab + b * SPAN + lax.broadcasted_iota(jnp.int32, (1, heads), 0) * 0
        seg_e = seg_of(edge + (SPAN - 1))
        seg_b = jnp.where(edge == 0, 0, seg_of(edge - 1))
        send = jnp.where(seg == seg_e, jnp.exp(end - cum), 0.0)
        read = jnp.where(seg == seg_b, jnp.exp(cum), 0.0)
        carry = jnp.where(seg_e == seg_b, jnp.exp(end), 0.0)
        f_in = read if back else send * dt
        fin_s[rows, :] = f_in
        fout_s[rows, :] = send * dt if back else read
        qt = [q_ref[rows, g * LANES:(g + 1) * LANES].T for g in range(groups)]
        for c in range(npair):
            cols = slice(c * LANES, (c + 1) * LANES)
            sent = (x_ref[rows, cols].astype(jnp.float32) * widen(f_in, c)).astype(jnp.bfloat16)
            loc = jnp.dot(qt[c // pair_group], sent, preferred_element_type=jnp.float32)
            wide = widen(carry, c)
            pre[step + 1, c] = wide * pre[step, c] + loc
            keep[step + 1, c] = wide * keep[step, c]

    def in_block():
        def one(b, _):
            start = pl.multiple_of(b * SPAN, SPAN)
            rows = pl.ds(start, SPAN)
            seg_i = seg_of(slab + start + dim0)
            seg_j = seg_of(slab + start + dim1)
            order = (dim1 >= dim0) if back else (dim1 <= dim0)
            bias = jnp.where((seg_i == seg_j) & order, 0.0, -jnp.inf)
            cum = cum_s[rows, :]
            dt = dt_ref[rows, :]
            f_out = fout_s[rows, :]
            for g in range(groups):
                gl = slice(g * LANES, (g + 1) * LANES)
                score = lax.dot_general(p_ref[rows, gl], q_ref[rows, gl], (((1,), (1,)), ((), ())),
                                        preferred_element_type=jnp.float32)
                for c in range(g * pair_group, (g + 1) * pair_group):
                    cols = slice(c * LANES, (c + 1) * LANES)
                    x = x_ref[rows, cols]
                    mixes, parts = [], []
                    for k in range(per):
                        h = c * per + k
                        col = cum[:, h:h + 1]
                        row = cum_t[b, h:h + 1, :]
                        spread = (row - col) if back else (col - row)
                        w = jnp.exp(spread + bias) * score
                        if not back:
                            w = w * dt_t[b, h:h + 1, :]
                        mixes.append(w.astype(jnp.bfloat16))
                        mine = (lane >= k * head_dim) & (lane < (k + 1) * head_dim)
                        parts.append(jnp.where(mine, x, jnp.zeros_like(x)))
                    acc = jnp.dot(jnp.concatenate(mixes, 1), jnp.concatenate(parts, 0),
                                  preferred_element_type=jnp.float32)
                    if back:
                        acc = acc * widen(dt, c)
                    inside[c, rows, :] = acc + widen(skip_ref[...], c) * x.astype(jnp.float32)
                    fexp[c, rows, :] = widen(f_out, c)
            return 0

        lax.fori_loop(0, nblocks, one, 0)

    def finish(c, _):
        for j in range(slices):
            src = c * slices + j

            @pl.when(src != me)
            def _():
                home(src).wait_recv()

        g = c // pair_group
        state = back_in[pl.ds(c * slices, slices)].reshape(LANES, LANES).astype(jnp.float32)
        cols = pl.ds(pl.multiple_of(c * LANES, LANES), LANES)
        gl = pl.ds(pl.multiple_of(g * LANES, LANES), LANES)
        for step in range(nblocks):
            b = nblocks - 1 - step if back else step
            rows = slice(b * SPAN, (b + 1) * SPAN)
            entering = (keep[step, c] * state + pre[step, c]).astype(jnp.bfloat16)
            y = jnp.dot(p_ref[rows, gl], entering, preferred_element_type=jnp.float32)
            out_ref[rows, cols] = (inside[c, rows, :] + fexp[c, rows, :] * y).astype(jnp.bfloat16)
        return 0

    def away(peer, slot):
        return pltpu.make_async_remote_copy(
            src_ref=give.at[peer], dst_ref=got.at[slot], send_sem=give_sem, recv_sem=got_sem.at[slot],
            device_id={"seq": peer}, device_id_type=MESH)

    def away_keep(peer, slot):
        return pltpu.make_async_remote_copy(
            src_ref=keep.at[nblocks, peer // slices], dst_ref=got_keep.at[slot], send_sem=keep_send,
            recv_sem=keep_recv, device_id={"seq": peer}, device_id_type=MESH)

    def home_to(peer, slot):
        return pltpu.make_async_remote_copy(
            src_ref=back_out.at[peer], dst_ref=back_in.at[slot], send_sem=out_sem, recv_sem=in_sem.at[slot],
            device_id={"seq": peer}, device_id_type=MESH)

    def home(src):
        return home_to(src, src)

    for c in range(npair):
        give[c * slices:(c + 1) * slices] = pre[nblocks, c].astype(jnp.bfloat16).reshape(slices, share, LANES)
    got[me] = give[me]
    got_keep[me] = keep[nblocks, me // slices]

    pl.semaphore_wait(barrier, count - 1)

    def send(k, _):
        peer = lax.rem(me + k, count)
        away_keep(peer, me).start()
        away(peer, me).start()
        return 0

    lax.fori_loop(1, count, send, 0)

    in_block()

    others = pl.ds(0, count - 1)
    pltpu.make_async_copy(got_keep.at[others], got_keep.at[others], keep_recv).wait()

    def scan(i, state):
        p = count - 1 - i if back else i

        @pl.when(p != me)
        def _():
            away(p, p).wait_recv()

        @pl.when(p != me)
        def _():
            back_out[p] = state.astype(jnp.bfloat16)
            home_to(p, me).start()

        @pl.when(p == me)
        def _():
            back_in[p] = state.astype(jnp.bfloat16)

        return got_keep[p] * state + got[p].astype(jnp.float32)

    lax.fori_loop(0, count, scan, jnp.zeros((share, LANES), jnp.float32))
    lax.fori_loop(0, npair, finish, 0)

    pltpu.make_async_copy(give.at[others], give.at[others], give_sem).wait()
    pltpu.make_async_copy(got_keep.at[others], got_keep.at[others], keep_send).wait()
    pltpu.make_async_copy(back_out.at[others], back_out.at[others], out_sem).wait()


def scan_pass(back, lengths, x, p_vec, q_vec, dt, decay, skip):
    tokens, width = x.shape
    heads = dt.shape[1]
    groups = p_vec.shape[1] // LANES
    head_dim = width // heads
    nblocks = tokens // SPAN
    npair = width // LANES
    count = lax.axis_size("seq")
    share = npair * LANES // count
    vm = pl.BlockSpec(memory_space=pltpu.VMEM)
    f32, bf16 = jnp.float32, jnp.bfloat16
    return pl.pallas_call(
        functools.partial(scan_kernel, back, count, nblocks, heads, groups, head_dim),
        out_shape=jax.ShapeDtypeStruct((tokens, width), bf16),
        in_specs=[pl.BlockSpec(memory_space=pltpu.SMEM)] + [vm] * 6,
        out_specs=vm,
        scratch_shapes=[
            pltpu.VMEM((tokens, heads), f32),
            pltpu.VMEM((nblocks, heads, SPAN), f32),
            pltpu.VMEM((nblocks, heads, SPAN), f32),
            pltpu.VMEM((tokens, heads), f32),
            pltpu.VMEM((tokens, heads), f32),
            pltpu.VMEM((npair, tokens, LANES), f32),
            pltpu.VMEM((npair, tokens, LANES), f32),
            pltpu.VMEM((nblocks + 1, npair, LANES, LANES), f32),
            pltpu.VMEM((nblocks + 1, npair, 1, LANES), f32),
            pltpu.VMEM((count, share, LANES), bf16),
            pltpu.VMEM((count, share, LANES), bf16),
            pltpu.VMEM((count, 1, LANES), f32),
            pltpu.VMEM((count, share, LANES), bf16),
            pltpu.VMEM((count, share, LANES), bf16),
            pltpu.SemaphoreType.DMA,
            pltpu.SemaphoreType.DMA((count,)),
            pltpu.SemaphoreType.DMA,
            pltpu.SemaphoreType.DMA,
            pltpu.SemaphoreType.DMA,
            pltpu.SemaphoreType.DMA((count,)),
        ],
        compiler_params=pltpu.CompilerParams(
            collective_id=1 if back else 0, has_side_effects=True,
            vmem_limit_bytes=40 * 1024 * 1024),
        cost_estimate=pl.CostEstimate(
            flops=40_000_000_000, bytes_accessed=8 * tokens * width, transcendentals=0),
        name="back_pass" if back else "next_pass",
    )(lengths, x, p_vec, q_vec, dt, decay, skip)


def body(
    hidden_next, values_next, seg_next, proj_bc, proj_dt, dt_bias, decay_rate, skip_gain,
    bc_prev, dt_prev, seg_prev, grad_prev,
):
    tokens_dev = hidden_next.shape[0]
    bc_width = proj_bc.shape[1]
    heads_all = proj_dt.shape[1]
    fsdp_count = lax.axis_size("fsdp")
    fsdp_place = lax.axis_index("fsdp")
    seq_count = lax.axis_size("seq")
    heads_dev = heads_all // fsdp_count
    state_dim = bc_width // (2 * GW)
    per_group = heads_all // GW
    groups_dev = max(1, heads_dev // per_group)
    first_head = fsdp_place * heads_dev
    first_group = first_head // per_group
    rows_dev = proj_bc.shape[0]
    half = bc_width // 2
    gw = groups_dev * state_dim

    pieces = []
    for f in range(fsdp_count):
        g0 = (f * heads_dev // per_group) * state_dim
        pieces += [proj_bc[:, g0:g0 + gw], proj_bc[:, half + g0:half + g0 + gw],
                   proj_dt[:, f * heads_dev:(f + 1) * heads_dev]]
    cols = 2 * gw + heads_dev
    weights = lax.all_gather(jnp.concatenate(pieces, axis=1), "seq", axis=0, tiled=True)

    decay = lax.dynamic_slice_in_dim(decay_rate, first_head, heads_dev, 0)[None]
    skip = lax.dynamic_slice_in_dim(skip_gain, first_head, heads_dev, 0)[None]
    bias = lax.dynamic_slice_in_dim(dt_bias, first_head, heads_dev, 0)[None]

    b_prev = lax.dynamic_slice_in_dim(bc_prev, first_group * state_dim, gw, 1)
    c_prev = lax.dynamic_slice_in_dim(bc_prev, half + first_group * state_dim, gw, 1)
    grad_values = scan_pass(True, seg_prev, grad_prev, b_prev, c_prev, dt_prev, decay, skip)

    owned = lax.dynamic_slice_in_dim(
        hidden_next.reshape(tokens_dev, seq_count, fsdp_count, rows_dev), fsdp_place, 1, 2
    ).reshape(tokens_dev, seq_count * rows_dev)
    owned, grad_values = lax.optimization_barrier((owned, grad_values))
    if fsdp_count == 2:
        other = lax.dynamic_slice_in_dim(weights, (1 - fsdp_place) * cols, cols, 1)
        mine = lax.dynamic_slice_in_dim(weights, fsdp_place * cols, cols, 1)
        away = lax.ppermute(jnp.dot(owned, other, preferred_element_type=jnp.float32),
                            "fsdp", [(0, 1), (1, 0)])
        sums = jnp.dot(owned, mine, preferred_element_type=jnp.float32) + away
    else:
        sums = lax.psum_scatter(jnp.dot(owned, weights, preferred_element_type=jnp.float32),
                                "fsdp", scatter_dimension=1, tiled=True)
    b_next = sums[:, :gw].astype(jnp.bfloat16)
    c_next = sums[:, gw:2 * gw].astype(jnp.bfloat16)
    dt_next = jax.nn.softplus(sums[:, 2 * gw:] + bias)
    out_next = scan_pass(False, seg_next, values_next, c_next, b_next, dt_next, decay, skip)
    return (out_next, grad_values)


def solution(mesh):
    in_specs = (
        P("seq", None), P("seq", "fsdp"), P(), P(("seq", "fsdp"), None), P(("seq", "fsdp"), None),
        P(), P(), P(), P("seq", None), P("seq", "fsdp"), P(), P("seq", "fsdp"),
    )
    out_specs = (P("seq", "fsdp"), P("seq", "fsdp"))
    return jax.shard_map(body, mesh=mesh, in_specs=in_specs, out_specs=out_specs, check_vma=False)
```

```python
import functools
import types

import jax
import jax.numpy as jnp
from jax import lax
from jax.experimental import pallas as pl
from jax.experimental.pallas import tpu as pltpu
from jax.sharding import PartitionSpec as P

SPAN = 128
LANES = 128
LEVEL = 4
MESH = pl.DeviceIdType.MESH
F32, BF16 = jnp.float32, jnp.bfloat16


def side_scratch(count, tokens, heads, npair, nblocks, share):
    return dict(
        cum_s=pltpu.VMEM((tokens, heads), F32),
        cum_t=pltpu.VMEM((nblocks, heads, SPAN), F32),
        dt_s=pltpu.VMEM((tokens, heads), F32),
        dt_t=pltpu.VMEM((nblocks, heads, SPAN), F32),
        fin_s=pltpu.VMEM((tokens, heads), F32),
        fout_s=pltpu.VMEM((tokens, heads), F32),
        carry=pltpu.VMEM((nblocks, npair, 1, LANES), F32),
        fexp=pltpu.VMEM((npair, tokens, LANES), F32),
        inside=pltpu.VMEM((npair, tokens, LANES), F32),
        pre=pltpu.VMEM((nblocks + 1, npair, LANES, LANES), F32),
        keep=pltpu.VMEM((nblocks + 1, npair, 1, LANES), F32),
        give=pltpu.VMEM((count, share, LANES), BF16),
        got=pltpu.VMEM((count, share, LANES), BF16),
        got_keep=pltpu.VMEM((count, 1, LANES), F32),
        back_out=pltpu.VMEM((count, share, LANES), BF16),
        back_in=pltpu.VMEM((count, share, LANES), BF16),
        give_sem=pltpu.SemaphoreType.DMA,
        got_sem=pltpu.SemaphoreType.DMA((count,)),
        keep_send=pltpu.SemaphoreType.DMA,
        keep_recv=pltpu.SemaphoreType.DMA,
        out_sem=pltpu.SemaphoreType.DMA,
        in_sem=pltpu.SemaphoreType.DMA((count,)),
    )


class Side:
    def __init__(self, back, me, count, dims, r, len_ref, x_ref, p_ref, q_ref, out_ref, decay_ref, skip_ref):
        self.back, self.me, self.count, self.r = back, me, count, r
        self.nblocks, self.heads, self.head_dim, self.npair = dims
        self.x, self.p, self.q, self.out = x_ref, p_ref, q_ref, out_ref
        self.decay, self.skip = decay_ref, skip_ref
        self.per = LANES // self.head_dim
        self.share = self.npair * LANES // count
        self.slices = LANES // self.share
        self.bound = []
        total = jnp.int32(0)
        for k in range(3):
            total = total + len_ref[k]
            self.bound.append(total)
        self.slab = me * (self.nblocks * SPAN)
        self.dim0 = lax.broadcasted_iota(jnp.int32, (SPAN, SPAN), 0)
        self.dim1 = lax.broadcasted_iota(jnp.int32, (SPAN, SPAN), 1)
        self.lane = lax.broadcasted_iota(jnp.int32, (1, LANES), 1)

    def seg_of(self, pos):
        s = jnp.zeros_like(pos)
        for b in self.bound:
            s = s + (b <= pos).astype(jnp.int32)
        return s

    def widen(self, a, c):
        res = a[:, c * self.per:c * self.per + 1]
        for k in range(1, self.per):
            res = jnp.where(self.lane >= k * self.head_dim, a[:, c * self.per + k:c * self.per + k + 1], res)
        return jnp.broadcast_to(res, (a.shape[0], LANES))

    def order(self):
        for step in range(self.nblocks):
            b = self.nblocks - 1 - step if self.back else step
            yield step, b, slice(b * SPAN, (b + 1) * SPAN)

    def factors(self, dt_of):
        r, heads = self.r, self.heads
        tril = (self.dim0 >= self.dim1).astype(F32)
        for c in range(self.npair):
            r.keep[0, c] = jnp.ones((1, LANES), F32)
        for step, b, rows in self.order():
            dt, dt_t = dt_of(b, rows)
            cum = jnp.dot(tril, -(dt * self.decay[...]), precision=lax.Precision.HIGHEST,
                          preferred_element_type=F32)
            end = cum[SPAN - 1:SPAN, :]
            r.cum_s[rows, :] = cum
            r.cum_t[b] = cum.T
            r.dt_s[rows, :] = dt
            r.dt_t[b] = dt_t
            pos = self.slab + b * SPAN + lax.broadcasted_iota(jnp.int32, (SPAN, heads), 0)
            seg = self.seg_of(pos)
            edge = self.slab + b * SPAN + lax.broadcasted_iota(jnp.int32, (1, heads), 0) * 0
            seg_e = self.seg_of(edge + (SPAN - 1))
            seg_b = jnp.where(edge == 0, 0, self.seg_of(edge - 1))
            send = jnp.where(seg == seg_e, jnp.exp(end - cum), 0.0) * dt
            read = jnp.where(seg == seg_b, jnp.exp(cum), 0.0)
            carry = jnp.where(seg_e == seg_b, jnp.exp(end), 0.0)
            r.fin_s[rows, :] = read if self.back else send
            r.fout_s[rows, :] = send if self.back else read
            for c in range(self.npair):
                wide = self.widen(carry, c)
                r.carry[step, c] = wide
                r.keep[step + 1, c] = wide * r.keep[step, c]
        r.got_keep[self.me] = r.keep[self.nblocks, self.me // self.slices]

    def locals(self):
        r, nblocks = self.r, self.nblocks
        for step, b, rows in self.order():
            qt = self.q[rows, :].T
            f_in = r.fin_s[rows, :]
            for c in range(self.npair):
                cols = slice(c * LANES, (c + 1) * LANES)
                sent = (self.x[rows, cols].astype(F32) * self.widen(f_in, c)).astype(BF16)
                loc = jnp.dot(qt, sent, preferred_element_type=F32)
                if step == 0:
                    r.pre[step, c] = jnp.zeros((LANES, LANES), F32)
                    r.pre[step + 1, c] = loc
                else:
                    r.pre[step + 1, c] = r.carry[step, c] * r.pre[step, c] + loc
        for c in range(self.npair):
            r.give[c * self.slices:(c + 1) * self.slices] = (
                r.pre[nblocks, c].astype(BF16).reshape(self.slices, self.share, LANES))
        r.got[self.me] = r.give[self.me]

    def away(self, peer, slot):
        r = self.r
        return pltpu.make_async_remote_copy(
            src_ref=r.give.at[peer], dst_ref=r.got.at[slot], send_sem=r.give_sem, recv_sem=r.got_sem.at[slot],
            device_id={"seq": peer}, device_id_type=MESH)

    def away_keep(self, peer, slot):
        r = self.r
        return pltpu.make_async_remote_copy(
            src_ref=r.keep.at[self.nblocks, peer // self.slices], dst_ref=r.got_keep.at[slot],
            send_sem=r.keep_send, recv_sem=r.keep_recv, device_id={"seq": peer}, device_id_type=MESH)

    def home(self, peer, slot):
        r = self.r
        return pltpu.make_async_remote_copy(
            src_ref=r.back_out.at[peer], dst_ref=r.back_in.at[slot], send_sem=r.out_sem,
            recv_sem=r.in_sem.at[slot], device_id={"seq": peer}, device_id_type=MESH)

    def send_keeps(self):
        def one(k, _):
            self.away_keep(lax.rem(self.me + k, self.count), self.me).start()
            return 0

        lax.fori_loop(1, self.count, one, 0)

    def send_locals(self):
        def one(k, _):
            self.away(lax.rem(self.me + k, self.count), self.me).start()
            return 0

        lax.fori_loop(1, self.count, one, 0)

    def in_block(self, b):
        r, per, head_dim = self.r, self.per, self.head_dim
        start = b * SPAN
        rows = slice(start, start + SPAN)
        seg_i = self.seg_of(self.slab + start + self.dim0)
        seg_j = self.seg_of(self.slab + start + self.dim1)
        ordered = (self.dim1 >= self.dim0) if self.back else (self.dim1 <= self.dim0)
        bias = jnp.where((seg_i == seg_j) & ordered, 0.0, -jnp.inf)
        cum = r.cum_s[rows, :]
        dt = r.dt_s[rows, :]
        f_out = r.fout_s[rows, :]
        score = lax.dot_general(self.p[rows, :], self.q[rows, :], (((1,), (1,)), ((), ())),
                                preferred_element_type=F32)
        for c in range(self.npair):
            cols = slice(c * LANES, (c + 1) * LANES)
            x = self.x[rows, cols]
            mixes, parts = [], []
            for k in range(per):
                h = c * per + k
                col = cum[:, h:h + 1]
                row = r.cum_t[b, h:h + 1, :]
                spread = (row - col) if self.back else (col - row)
                w = jnp.exp(spread + bias) * score
                if not self.back:
                    w = w * r.dt_t[b, h:h + 1, :]
                mixes.append(w.astype(BF16))
                mine = (self.lane >= k * head_dim) & (self.lane < (k + 1) * head_dim)
                parts.append(jnp.where(mine, x, jnp.zeros_like(x)))
            acc = jnp.dot(jnp.concatenate(mixes, 1), jnp.concatenate(parts, 0), preferred_element_type=F32)
            if self.back:
                acc = acc * self.widen(dt, c)
            r.inside[c, rows, :] = acc + self.widen(self.skip[...], c) * x.astype(F32)
            r.fexp[c, rows, :] = self.widen(f_out, c)

    def scan(self):
        r, me, count = self.r, self.me, self.count
        others = pl.ds(0, count - 1)
        pltpu.make_async_copy(r.got_keep.at[others], r.got_keep.at[others], r.keep_recv).wait()

        def one(i, state):
            p = count - 1 - i if self.back else i

            @pl.when(p != me)
            def _():
                self.away(p, p).wait_recv()
                r.back_out[p] = state.astype(BF16)
                self.home(p, me).start()

            @pl.when(p == me)
            def _():
                r.back_in[p] = state.astype(BF16)

            return r.got_keep[p] * state + r.got[p].astype(F32)

        lax.fori_loop(0, count, one, jnp.zeros((self.share, LANES), F32))

    def finish(self):
        r, me, slices = self.r, self.me, self.slices

        def one(c, _):
            for j in range(slices):
                src = c * slices + j

                @pl.when(src != me)
                def _():
                    self.home(src, src).wait_recv()

            state = r.back_in[pl.ds(c * slices, slices)].reshape(LANES, LANES).astype(F32)
            cols = pl.ds(pl.multiple_of(c * LANES, LANES), LANES)
            for step, b, rows in self.order():
                entering = (r.keep[step, c] * state + r.pre[step, c]).astype(BF16)
                y = jnp.dot(self.p[rows, :], entering, preferred_element_type=F32)
                self.out[rows, cols] = (r.inside[c, rows, :] + r.fexp[c, rows, :] * y).astype(BF16)
            return 0

        lax.fori_loop(0, self.npair, one, 0)

    def drain(self):
        r = self.r
        others = pl.ds(0, self.count - 1)
        pltpu.make_async_copy(r.give.at[others], r.give.at[others], r.give_sem).wait()
        pltpu.make_async_copy(r.got_keep.at[others], r.got_keep.at[others], r.keep_send).wait()
        pltpu.make_async_copy(r.back_out.at[others], r.back_out.at[others], r.out_sem).wait()


def layer_kernel(names, count, nfsdp, dims, *refs):
    r = types.SimpleNamespace(**dict(zip(names, refs)))
    nblocks, heads, head_dim, npair = dims
    me = lax.axis_index("seq")
    fs = lax.axis_index("fsdp")
    part = lax.rem(fs, 2)
    group = fs // 2
    half = r.proj_bc.shape[1] // 2
    rows_dev = r.proj_bc.shape[0]
    tall = nfsdp * rows_dev
    nlevels = count // LEVEL

    barrier = pltpu.get_barrier_semaphore()

    def greet_seq(k, _):
        pl.semaphore_signal(barrier, inc=1, device_id={"seq": lax.rem(me + k, count)}, device_id_type=MESH)
        return 0

    def greet_fsdp(k, _):
        pl.semaphore_signal(barrier, inc=1, device_id={"fsdp": lax.rem(fs + k, nfsdp)}, device_id_type=MESH)
        return 0

    lax.fori_loop(1, nfsdp, greet_fsdp, 0)
    lax.fori_loop(1, count, greet_seq, 0)

    bcol = pl.ds(pl.multiple_of(group * LANES, LANES), LANES)
    ccol = pl.ds(pl.multiple_of(half + group * LANES, LANES), LANES)
    loads = [
        pltpu.make_async_copy(r.grad_hbm, r.grad_v, r.load_sem.at[0]),
        pltpu.make_async_copy(r.bc_prev.at[:, ccol], r.c_prev, r.load_sem.at[1]),
        pltpu.make_async_copy(r.bc_prev.at[:, bcol], r.b_prev, r.load_sem.at[2]),
        pltpu.make_async_copy(r.values_hbm, r.values_v, r.load_sem.at[3]),
        pltpu.make_async_copy(r.hidden_hbm, r.hidden_v, r.load_sem.at[4]),
    ]
    for load in loads:
        load.start()

    def sub(prefix):
        return types.SimpleNamespace(**{k[len(prefix):]: v for k, v in vars(r).items() if k.startswith(prefix)})

    prev = Side(True, me, count, dims, sub("prev_"), r.seg_prev, r.grad_v, r.b_prev, r.c_prev, r.grad_values,
                r.decay, r.skip)
    nxt = Side(False, me, count, dims, sub("next_"), r.seg_next, r.values_v, r.bc_new.at[1], r.bc_new.at[0],
               r.out_next, r.decay, r.skip)

    def dt_prev_of(b, rows):
        dt_t = r.dt_prev_t[:, rows]
        return dt_t.T, dt_t

    prev.factors(dt_prev_of)
    loads[0].wait()
    loads[1].wait()
    prev.locals()

    pl.semaphore_wait(barrier, count + nfsdp - 2)

    def cols_for(peer):
        return pl.ds(pl.multiple_of(lax.rem(peer, 2) * half + (peer // 2) * LANES, LANES), LANES)

    def hand_bc(peer, slot):
        at = pl.ds(pl.multiple_of(slot * rows_dev, rows_dev), rows_dev)
        return pltpu.make_async_remote_copy(
            src_ref=r.proj_bc.at[:, cols_for(peer)], dst_ref=r.weights.at[me, at], send_sem=r.hand_send.at[0],
            recv_sem=r.hand_recv.at[0], device_id={"fsdp": peer}, device_id_type=MESH)

    def hand_dt(peer, slot):
        return pltpu.make_async_remote_copy(
            src_ref=r.proj_dt, dst_ref=r.dt_rows.at[slot], send_sem=r.hand_send.at[1],
            recv_sem=r.hand_recv.at[1], device_id={"fsdp": peer}, device_id_type=MESH)

    def hand(k, _):
        peer = lax.rem(fs + k, nfsdp)
        hand_bc(peer, fs).start()
        hand_dt(peer, fs).start()
        return 0

    lax.fori_loop(1, nfsdp, hand, 0)
    r.weights[me, pl.ds(pl.multiple_of(fs * rows_dev, rows_dev), rows_dev), :] = r.proj_bc[:, cols_for(fs)]
    r.dt_rows[fs] = r.proj_dt[...]

    prev.send_keeps()
    prev.send_locals()
    loads[2].wait()
    prev.in_block(0)

    most = pl.ds(0, (nfsdp - 1) * rows_dev)
    pltpu.make_async_copy(r.weights.at[me, most], r.weights.at[me, most], r.hand_recv.at[0]).wait()
    pltpu.make_async_copy(r.dt_rows.at[pl.ds(0, nfsdp - 1)], r.dt_rows.at[pl.ds(0, nfsdp - 1)],
                          r.hand_recv.at[1]).wait()
    lane = lax.broadcasted_iota(jnp.int32, (rows_dev, LANES), 1)
    packed = jnp.zeros((rows_dev, LANES), F32)
    for g in range(nfsdp):
        turn = lax.rem((g - fs + nfsdp) * heads, LANES)
        moved = pltpu.roll(r.dt_rows[g].astype(F32), turn, 1)
        packed = jnp.where(lane // heads == g, moved, packed)
    r.weights[me, tall:tall + rows_dev, :] = packed.astype(BF16)

    up = lax.rem(me + LEVEL, count)
    down = lax.rem(me + count - LEVEL, count)
    sib = me + 1 - 2 * lax.rem(me, 2)
    other_x = me + 2 - 4 * lax.rem(me // 2, 2)

    def chunk(src, to):
        return pltpu.make_async_remote_copy(
            src_ref=r.weights.at[src], dst_ref=r.weights.at[src], send_sem=r.ring_send,
            recv_sem=r.ring_recv.at[src], device_id={"seq": to}, device_id_type=MESH)

    def at(base, k):
        return lax.rem(base + (count + k * LEVEL), count)

    def relay(src, *targets):
        chunk(src, sib).wait_recv()
        for to in targets:
            chunk(src, to).start()

    for to in (up, down, other_x, sib):
        chunk(me, to).start()

    def level(k, first=False):
        z = lax.rem(me // LEVEL + nlevels + k, nlevels)
        chunk(at(sib, k), sib).wait_recv()
        chunk(at(sib + other_x - me, k), sib).wait_recv()
        lhs = r.hidden_v[:, pl.ds(pl.multiple_of(z * LEVEL * tall, LEVEL * tall), LEVEL * tall)]
        row = lax.broadcasted_iota(jnp.int32, (tall, LANES), 0)
        col = lax.broadcasted_iota(jnp.int32, (tall, LANES), 1)
        own = (row // rows_dev) == (col // heads)
        tiles = []
        for j in range(LEVEL):
            s = z * LEVEL + j
            dt_w = r.weights[s, tall:tall + rows_dev, :]
            spread = jnp.concatenate([dt_w] * nfsdp, 0)
            tiles.append(jnp.concatenate(
                [r.weights[s, 0:tall, :], jnp.where(own, spread, jnp.zeros_like(spread))], 1))
        res = jnp.dot(lhs, jnp.concatenate(tiles, 0), preferred_element_type=F32)
        r.sums[...] = res if first else r.sums[...] + res

    prev.in_block(1)
    relay(at(me, -1), up, other_x, sib)
    relay(at(me, 1), down, other_x, sib)
    relay(other_x, sib)
    prev.scan()
    relay(at(me, -2), up, other_x, sib)
    relay(at(me, 2), down, other_x, sib)
    relay(at(other_x, -1), sib)
    relay(at(other_x, 1), sib)
    loads[4].wait()
    level(0, first=True)
    relay(at(me, -3), up, other_x, sib)
    relay(at(me, 3), other_x, sib)
    relay(at(other_x, -2), sib)
    relay(at(other_x, 2), sib)
    level(-1)
    level(1)
    relay(at(me, -4), other_x, sib)
    relay(at(other_x, -3), sib)
    relay(at(other_x, 3), sib)
    level(-2)
    level(2)
    relay(at(other_x, -4), sib)
    level(-3)
    level(3)
    level(-4)

    mate = fs + 1 - 2 * part
    r.bc_new[part] = r.sums[:, 0:LANES].astype(BF16)
    swap = pltpu.make_async_remote_copy(
        src_ref=r.bc_new.at[part], dst_ref=r.bc_new.at[part], send_sem=r.swap_send, recv_sem=r.swap_recv,
        device_id={"fsdp": mate}, device_id_type=MESH)
    swap.start()

    def dt_next_of(b, rows):
        v = r.sums[rows, LANES:2 * LANES]
        turn = LANES // 2
        while turn >= heads:
            v = v + pltpu.roll(v, turn, 1)
            turn //= 2
        v = v[:, 0:heads] + r.dt_bias[...]
        dt = jnp.maximum(v, 0.0) + jnp.log1p(jnp.exp(-jnp.abs(v)))
        return dt, dt.T

    nxt.factors(dt_next_of)
    nxt.send_keeps()
    loads[3].wait()
    swap.wait_recv()
    nxt.locals()
    nxt.send_locals()
    for b in range(nblocks):
        nxt.in_block(b)
    prev.finish()
    nxt.scan()
    nxt.finish()

    prev.drain()
    nxt.drain()
    swap.wait_send()
    pltpu.make_async_copy(r.weights.at[0, most], r.weights.at[0, most], r.hand_send.at[0]).wait()
    pltpu.make_async_copy(r.dt_rows.at[pl.ds(0, nfsdp - 1)], r.dt_rows.at[pl.ds(0, nfsdp - 1)],
                          r.hand_send.at[1]).wait()
    pltpu.make_async_copy(r.weights.at[pl.ds(0, count - 1)], r.weights.at[pl.ds(0, count - 1)], r.ring_send).wait()


def body(
    hidden_next, values_next, seg_next, proj_bc, proj_dt, dt_bias, decay_rate, skip_gain,
    bc_prev, dt_prev, seg_prev, grad_prev,
):
    tokens, width = values_next.shape
    nfsdp = lax.axis_size("fsdp")
    count = lax.axis_size("seq")
    heads = proj_dt.shape[1] // nfsdp
    head_dim = width // heads
    npair = width // LANES
    nblocks = tokens // SPAN
    share = npair * LANES // count
    rows_dev = proj_bc.shape[0]
    tall = nfsdp * rows_dev
    first_head = lax.axis_index("fsdp") * heads

    def mine(v):
        return lax.dynamic_slice_in_dim(v, first_head, heads, 0)[None]

    vm, sm, hbm = (pl.BlockSpec(memory_space=s) for s in (pltpu.VMEM, pltpu.SMEM, pl.ANY))
    ins = dict(
        seg_next=(seg_next, sm), seg_prev=(seg_prev, sm),
        proj_bc=(proj_bc, vm), proj_dt=(proj_dt, vm),
        dt_bias=(mine(dt_bias), vm), decay=(mine(decay_rate), vm), skip=(mine(skip_gain), vm),
        dt_prev_t=(dt_prev.T, vm),
        hidden_hbm=(hidden_next, hbm), values_hbm=(values_next, hbm), grad_hbm=(grad_prev, hbm),
        bc_prev=(bc_prev, hbm),
    )
    scratch = dict(
        grad_v=pltpu.VMEM((tokens, width), BF16),
        values_v=pltpu.VMEM((tokens, width), BF16),
        hidden_v=pltpu.VMEM(hidden_next.shape, BF16),
        b_prev=pltpu.VMEM((tokens, LANES), BF16),
        c_prev=pltpu.VMEM((tokens, LANES), BF16),
        weights=pltpu.VMEM((count, tall + rows_dev, LANES), BF16),
        dt_rows=pltpu.VMEM((nfsdp, rows_dev, LANES), BF16),
        sums=pltpu.VMEM((tokens, 2 * LANES), F32),
        bc_new=pltpu.VMEM((2, tokens, LANES), BF16),
        load_sem=pltpu.SemaphoreType.DMA((5,)),
        hand_send=pltpu.SemaphoreType.DMA((2,)),
        hand_recv=pltpu.SemaphoreType.DMA((2,)),
        ring_send=pltpu.SemaphoreType.DMA,
        ring_recv=pltpu.SemaphoreType.DMA((count,)),
        swap_send=pltpu.SemaphoreType.DMA,
        swap_recv=pltpu.SemaphoreType.DMA,
    )
    for name in ("prev", "next"):
        for key, val in side_scratch(count, tokens, heads, npair, nblocks, share).items():
            scratch[f"{name}_{key}"] = val
    names = list(ins) + ["out_next", "grad_values"] + list(scratch)
    out = jax.ShapeDtypeStruct((tokens, width), BF16)
    return pl.pallas_call(
        functools.partial(layer_kernel, names, count, nfsdp, (nblocks, heads, head_dim, npair)),
        out_shape=(out, out),
        in_specs=[spec for _, spec in ins.values()],
        out_specs=(vm, vm),
        scratch_shapes=list(scratch.values()),
        compiler_params=pltpu.CompilerParams(
            collective_id=0, has_side_effects=True, vmem_limit_bytes=60 * 1024 * 1024),
        cost_estimate=pl.CostEstimate(flops=4_000_000_000, bytes_accessed=16 * tokens * width, transcendentals=0),
        name="layer",
    )(*[val for val, _ in ins.values()])


def solution(mesh):
    in_specs = (
        P("seq", None), P("seq", "fsdp"), P(), P(("seq", "fsdp"), None), P(("seq", "fsdp"), None),
        P(), P(), P(), P("seq", None), P("seq", "fsdp"), P(), P("seq", "fsdp"),
    )
    out_specs = (P("seq", "fsdp"), P("seq", "fsdp"))
    return jax.shard_map(body, mesh=mesh, in_specs=in_specs, out_specs=out_specs, check_vma=False)
```

```python
import functools
import types

import jax
import jax.numpy as jnp
from jax import lax
from jax.experimental import pallas as pl
from jax.experimental.pallas import tpu as pltpu
from jax.sharding import PartitionSpec as P

SPAN = 128
LANES = 128
LEVEL = 4
MESH = pl.DeviceIdType.MESH
F32, BF16 = jnp.float32, jnp.bfloat16


def side_scratch(count, tokens, heads, npair, nblocks, share):
    return dict(
        cum_s=pltpu.VMEM((tokens, heads), F32),
        cum_t=pltpu.VMEM((nblocks, heads, SPAN), F32),
        dt_s=pltpu.VMEM((tokens, heads), F32),
        dt_t=pltpu.VMEM((nblocks, heads, SPAN), F32),
        fin_s=pltpu.VMEM((tokens, heads), F32),
        fout_s=pltpu.VMEM((tokens, heads), F32),
        carry=pltpu.VMEM((nblocks, npair, 1, LANES), F32),
        fexp=pltpu.VMEM((npair, tokens, LANES), F32),
        inside=pltpu.VMEM((npair, tokens, LANES), F32),
        pre=pltpu.VMEM((nblocks + 1, npair, LANES, LANES), F32),
        keep=pltpu.VMEM((nblocks + 1, npair, 1, LANES), F32),
        give=pltpu.VMEM((count, share, LANES), BF16),
        got=pltpu.VMEM((count, share, LANES), BF16),
        got_keep=pltpu.VMEM((count, 1, LANES), F32),
        back_out=pltpu.VMEM((count, share, LANES), BF16),
        back_in=pltpu.VMEM((count, share, LANES), BF16),
        give_sem=pltpu.SemaphoreType.DMA,
        got_sem=pltpu.SemaphoreType.DMA((count,)),
        keep_send=pltpu.SemaphoreType.DMA,
        keep_recv=pltpu.SemaphoreType.DMA,
        out_sem=pltpu.SemaphoreType.DMA,
        in_sem=pltpu.SemaphoreType.DMA((count,)),
    )


class Side:
    def __init__(self, back, me, count, dims, r, len_ref, x_ref, p_ref, q_ref, out_ref, decay_ref, skip_ref):
        self.back, self.me, self.count, self.r = back, me, count, r
        self.nblocks, self.heads, self.head_dim, self.npair = dims
        self.x, self.p, self.q, self.out = x_ref, p_ref, q_ref, out_ref
        self.decay, self.skip = decay_ref, skip_ref
        self.per = LANES // self.head_dim
        self.share = self.npair * LANES // count
        self.slices = LANES // self.share
        self.bound = []
        total = jnp.int32(0)
        for k in range(3):
            total = total + len_ref[k]
            self.bound.append(total)
        self.slab = me * (self.nblocks * SPAN)
        self.dim0 = lax.broadcasted_iota(jnp.int32, (SPAN, SPAN), 0)
        self.dim1 = lax.broadcasted_iota(jnp.int32, (SPAN, SPAN), 1)
        self.lane = lax.broadcasted_iota(jnp.int32, (1, LANES), 1)

    def seg_of(self, pos):
        s = jnp.zeros_like(pos)
        for b in self.bound:
            s = s + (b <= pos).astype(jnp.int32)
        return s

    def widen(self, a, c):
        res = a[:, c * self.per:c * self.per + 1]
        for k in range(1, self.per):
            res = jnp.where(self.lane >= k * self.head_dim, a[:, c * self.per + k:c * self.per + k + 1], res)
        return jnp.broadcast_to(res, (a.shape[0], LANES))

    def order(self):
        for step in range(self.nblocks):
            b = self.nblocks - 1 - step if self.back else step
            yield step, b, slice(b * SPAN, (b + 1) * SPAN)

    def factors(self, dt_of):
        r, heads = self.r, self.heads
        tril = (self.dim0 >= self.dim1).astype(F32)
        for c in range(self.npair):
            r.keep[0, c] = jnp.ones((1, LANES), F32)
        for step, b, rows in self.order():
            dt, dt_t = dt_of(b, rows)
            cum = jnp.dot(tril, -(dt * self.decay[...]), precision=lax.Precision.HIGHEST,
                          preferred_element_type=F32)
            end = cum[SPAN - 1:SPAN, :]
            r.cum_s[rows, :] = cum
            r.cum_t[b] = cum.T
            r.dt_s[rows, :] = dt
            r.dt_t[b] = dt_t
            pos = self.slab + b * SPAN + lax.broadcasted_iota(jnp.int32, (SPAN, heads), 0)
            seg = self.seg_of(pos)
            edge = self.slab + b * SPAN + lax.broadcasted_iota(jnp.int32, (1, heads), 0) * 0
            seg_e = self.seg_of(edge + (SPAN - 1))
            seg_b = jnp.where(edge == 0, 0, self.seg_of(edge - 1))
            send = jnp.where(seg == seg_e, jnp.exp(end - cum), 0.0) * dt
            read = jnp.where(seg == seg_b, jnp.exp(cum), 0.0)
            carry = jnp.where(seg_e == seg_b, jnp.exp(end), 0.0)
            r.fin_s[rows, :] = read if self.back else send
            r.fout_s[rows, :] = send if self.back else read
            for c in range(self.npair):
                wide = self.widen(carry, c)
                r.carry[step, c] = wide
                r.keep[step + 1, c] = wide * r.keep[step, c]
        r.got_keep[self.me] = r.keep[self.nblocks, self.me // self.slices]

    def locals(self):
        r, nblocks = self.r, self.nblocks
        for step, b, rows in self.order():
            qt = self.q[rows, :].T
            f_in = r.fin_s[rows, :]
            for c in range(self.npair):
                cols = slice(c * LANES, (c + 1) * LANES)
                sent = (self.x[rows, cols].astype(F32) * self.widen(f_in, c)).astype(BF16)
                loc = jnp.dot(qt, sent, preferred_element_type=F32)
                if step == 0:
                    r.pre[step, c] = jnp.zeros((LANES, LANES), F32)
                    r.pre[step + 1, c] = loc
                else:
                    r.pre[step + 1, c] = r.carry[step, c] * r.pre[step, c] + loc
        for c in range(self.npair):
            r.give[c * self.slices:(c + 1) * self.slices] = (
                r.pre[nblocks, c].astype(BF16).reshape(self.slices, self.share, LANES))
        r.got[self.me] = r.give[self.me]

    def away(self, peer, slot):
        r = self.r
        return pltpu.make_async_remote_copy(
            src_ref=r.give.at[peer], dst_ref=r.got.at[slot], send_sem=r.give_sem, recv_sem=r.got_sem.at[slot],
            device_id={"seq": peer}, device_id_type=MESH)

    def away_keep(self, peer, slot):
        r = self.r
        return pltpu.make_async_remote_copy(
            src_ref=r.keep.at[self.nblocks, peer // self.slices], dst_ref=r.got_keep.at[slot],
            send_sem=r.keep_send, recv_sem=r.keep_recv, device_id={"seq": peer}, device_id_type=MESH)

    def home(self, peer, slot):
        r = self.r
        return pltpu.make_async_remote_copy(
            src_ref=r.back_out.at[peer], dst_ref=r.back_in.at[slot], send_sem=r.out_sem,
            recv_sem=r.in_sem.at[slot], device_id={"seq": peer}, device_id_type=MESH)

    def send_keeps(self):
        def one(k, _):
            self.away_keep(lax.rem(self.me + k, self.count), self.me).start()
            return 0

        lax.fori_loop(1, self.count, one, 0)

    def send_locals(self):
        def one(k, _):
            self.away(lax.rem(self.me + k, self.count), self.me).start()
            return 0

        lax.fori_loop(1, self.count, one, 0)

    def in_block(self, b):
        r, per, head_dim = self.r, self.per, self.head_dim
        start = b * SPAN
        rows = slice(start, start + SPAN)
        seg_i = self.seg_of(self.slab + start + self.dim0)
        seg_j = self.seg_of(self.slab + start + self.dim1)
        ordered = (self.dim1 >= self.dim0) if self.back else (self.dim1 <= self.dim0)
        bias = jnp.where((seg_i == seg_j) & ordered, 0.0, -jnp.inf)
        cum = r.cum_s[rows, :]
        dt = r.dt_s[rows, :]
        f_out = r.fout_s[rows, :]
        score = lax.dot_general(self.p[rows, :], self.q[rows, :], (((1,), (1,)), ((), ())),
                                preferred_element_type=F32)
        for c in range(self.npair):
            cols = slice(c * LANES, (c + 1) * LANES)
            x = self.x[rows, cols]
            mixes, parts = [], []
            for k in range(per):
                h = c * per + k
                col = cum[:, h:h + 1]
                row = r.cum_t[b, h:h + 1, :]
                spread = (row - col) if self.back else (col - row)
                w = jnp.exp(spread + bias) * score
                if not self.back:
                    w = w * r.dt_t[b, h:h + 1, :]
                mixes.append(w.astype(BF16))
                mine = (self.lane >= k * head_dim) & (self.lane < (k + 1) * head_dim)
                parts.append(jnp.where(mine, x, jnp.zeros_like(x)))
            acc = jnp.dot(jnp.concatenate(mixes, 1), jnp.concatenate(parts, 0), preferred_element_type=F32)
            if self.back:
                acc = acc * self.widen(dt, c)
            r.inside[c, rows, :] = acc + self.widen(self.skip[...], c) * x.astype(F32)
            r.fexp[c, rows, :] = self.widen(f_out, c)

    def scan(self):
        r, me, count = self.r, self.me, self.count
        others = pl.ds(0, count - 1)
        pltpu.make_async_copy(r.got_keep.at[others], r.got_keep.at[others], r.keep_recv).wait()

        def one(i, state):
            p = count - 1 - i if self.back else i

            @pl.when(p != me)
            def _():
                self.away(p, p).wait_recv()
                r.back_out[p] = state.astype(BF16)
                self.home(p, me).start()

            @pl.when(p == me)
            def _():
                r.back_in[p] = state.astype(BF16)

            return r.got_keep[p] * state + r.got[p].astype(F32)

        lax.fori_loop(0, count, one, jnp.zeros((self.share, LANES), F32))

    def finish(self):
        r, me, slices = self.r, self.me, self.slices

        def one(c, _):
            for j in range(slices):
                src = c * slices + j

                @pl.when(src != me)
                def _():
                    self.home(src, src).wait_recv()

            state = r.back_in[pl.ds(c * slices, slices)].reshape(LANES, LANES).astype(F32)
            cols = pl.ds(pl.multiple_of(c * LANES, LANES), LANES)
            for step, b, rows in self.order():
                entering = (r.keep[step, c] * state + r.pre[step, c]).astype(BF16)
                y = jnp.dot(self.p[rows, :], entering, preferred_element_type=F32)
                self.out[rows, cols] = (r.inside[c, rows, :] + r.fexp[c, rows, :] * y).astype(BF16)
            return 0

        lax.fori_loop(0, self.npair, one, 0)

    def drain(self):
        r = self.r
        others = pl.ds(0, self.count - 1)
        pltpu.make_async_copy(r.give.at[others], r.give.at[others], r.give_sem).wait()
        pltpu.make_async_copy(r.got_keep.at[others], r.got_keep.at[others], r.keep_send).wait()
        pltpu.make_async_copy(r.back_out.at[others], r.back_out.at[others], r.out_sem).wait()


def layer_kernel(names, count, nfsdp, dims, *refs):
    r = types.SimpleNamespace(**dict(zip(names, refs)))
    nblocks, heads, head_dim, npair = dims
    me = lax.axis_index("seq")
    fs = lax.axis_index("fsdp")
    part = lax.rem(fs, 2)
    group = fs // 2
    half = r.proj_bc.shape[1] // 2
    rows_dev = r.proj_bc.shape[0]
    tall = nfsdp * rows_dev
    nlevels = count // LEVEL

    barrier = pltpu.get_barrier_semaphore()

    def greet_seq(k, _):
        pl.semaphore_signal(barrier, inc=1, device_id={"seq": lax.rem(me + k, count)}, device_id_type=MESH)
        return 0

    def greet_fsdp(k, _):
        pl.semaphore_signal(barrier, inc=1, device_id={"fsdp": lax.rem(fs + k, nfsdp)}, device_id_type=MESH)
        return 0

    first = [
        pltpu.make_async_copy(r.proj_bc_hbm, r.proj_bc, r.load_sem.at[0]),
        pltpu.make_async_copy(r.proj_dt_hbm, r.proj_dt, r.load_sem.at[1]),
    ]
    lengths = [
        pltpu.make_async_copy(r.seg_prev_hbm, r.seg_prev, r.load_sem.at[11]),
        pltpu.make_async_copy(r.seg_next_hbm, r.seg_next, r.load_sem.at[12]),
    ]
    for load in first + lengths:
        load.start()
    lax.fori_loop(1, nfsdp, greet_fsdp, 0)
    lax.fori_loop(1, count, greet_seq, 0)

    bcol = pl.ds(pl.multiple_of(group * LANES, LANES), LANES)
    ccol = pl.ds(pl.multiple_of(half + group * LANES, LANES), LANES)
    loads = [
        pltpu.make_async_copy(r.dt_prev_hbm, r.dt_prev_t, r.load_sem.at[2]),
        pltpu.make_async_copy(r.decay_hbm, r.heads_v.at[0], r.load_sem.at[3]),
        pltpu.make_async_copy(r.skip_hbm, r.heads_v.at[1], r.load_sem.at[4]),
        pltpu.make_async_copy(r.bias_hbm, r.heads_v.at[2], r.load_sem.at[5]),
        pltpu.make_async_copy(r.grad_hbm, r.grad_v, r.load_sem.at[6]),
        pltpu.make_async_copy(r.bc_prev.at[:, ccol], r.c_prev, r.load_sem.at[7]),
        pltpu.make_async_copy(r.bc_prev.at[:, bcol], r.b_prev, r.load_sem.at[8]),
        pltpu.make_async_copy(r.values_hbm, r.values_v, r.load_sem.at[9]),
        pltpu.make_async_copy(r.hidden_hbm, r.hidden_v, r.load_sem.at[10]),
    ]
    for load in loads:
        load.start()

    for load in lengths:
        load.wait()

    def sub(prefix):
        return types.SimpleNamespace(**{k[len(prefix):]: v for k, v in vars(r).items() if k.startswith(prefix)})

    prev = Side(True, me, count, dims, sub("prev_"), r.seg_prev, r.grad_v, r.b_prev, r.c_prev, r.grad_values,
                r.mine_v.at[0], r.mine_v.at[1])
    nxt = Side(False, me, count, dims, sub("next_"), r.seg_next, r.values_v, r.bc_new.at[1], r.bc_new.at[0],
               r.out_next, r.mine_v.at[0], r.mine_v.at[1])

    def dt_prev_of(b, rows):
        dt_t = r.dt_prev_t[:, rows]
        return dt_t.T, dt_t

    pl.semaphore_wait(barrier, count + nfsdp - 2)

    def cols_for(peer):
        return pl.ds(pl.multiple_of(lax.rem(peer, 2) * half + (peer // 2) * LANES, LANES), LANES)

    def hand_bc(peer, slot):
        at = pl.ds(pl.multiple_of(slot * rows_dev, rows_dev), rows_dev)
        return pltpu.make_async_remote_copy(
            src_ref=r.proj_bc.at[:, cols_for(peer)], dst_ref=r.weights.at[me, at], send_sem=r.hand_send.at[0],
            recv_sem=r.hand_recv.at[0], device_id={"fsdp": peer}, device_id_type=MESH)

    def hand_dt(peer, slot):
        return pltpu.make_async_remote_copy(
            src_ref=r.proj_dt, dst_ref=r.dt_rows.at[slot], send_sem=r.hand_send.at[1],
            recv_sem=r.hand_recv.at[1], device_id={"fsdp": peer}, device_id_type=MESH)

    def hand(k, _):
        peer = lax.rem(fs + k, nfsdp)
        hand_bc(peer, fs).start()
        hand_dt(peer, fs).start()
        return 0

    for load in first:
        load.wait()
    lax.fori_loop(1, nfsdp, hand, 0)
    r.weights[me, pl.ds(pl.multiple_of(fs * rows_dev, rows_dev), rows_dev), :] = r.proj_bc[:, cols_for(fs)]
    r.dt_rows[fs] = r.proj_dt[...]

    for load in loads[:4]:
        load.wait()
    for k in range(3):
        turned = pltpu.roll(jnp.broadcast_to(r.heads_v[k], (8, LANES)), lax.rem(LANES - fs * heads, LANES), 1)
        r.mine_v[k] = turned[0:1, 0:heads]
    prev.factors(dt_prev_of)
    prev.send_keeps()
    loads[4].wait()
    loads[5].wait()
    prev.locals()
    prev.send_locals()
    loads[6].wait()
    prev.in_block(0)

    most = pl.ds(0, (nfsdp - 1) * rows_dev)
    pltpu.make_async_copy(r.weights.at[me, most], r.weights.at[me, most], r.hand_recv.at[0]).wait()
    pltpu.make_async_copy(r.dt_rows.at[pl.ds(0, nfsdp - 1)], r.dt_rows.at[pl.ds(0, nfsdp - 1)],
                          r.hand_recv.at[1]).wait()
    lane = lax.broadcasted_iota(jnp.int32, (rows_dev, LANES), 1)
    packed = jnp.zeros((rows_dev, LANES), F32)
    for g in range(nfsdp):
        turn = lax.rem((g - fs + nfsdp) * heads, LANES)
        moved = pltpu.roll(r.dt_rows[g].astype(F32), turn, 1)
        packed = jnp.where(lane // heads == g, moved, packed)
    r.weights[me, tall:tall + rows_dev, :] = packed.astype(BF16)

    up = lax.rem(me + LEVEL, count)
    down = lax.rem(me + count - LEVEL, count)
    sib = me + 1 - 2 * lax.rem(me, 2)
    other_x = me + 2 - 4 * lax.rem(me // 2, 2)

    def chunk(src, to):
        return pltpu.make_async_remote_copy(
            src_ref=r.weights.at[src], dst_ref=r.weights.at[src], send_sem=r.ring_send,
            recv_sem=r.ring_recv.at[src], device_id={"seq": to}, device_id_type=MESH)

    def at(base, k):
        return lax.rem(base + (count + k * LEVEL), count)

    def relay(src, *targets):
        chunk(src, sib).wait_recv()
        for to in targets:
            chunk(src, to).start()

    for to in (up, down, other_x, sib):
        chunk(me, to).start()

    def level(k, first=False):
        z = lax.rem(me // LEVEL + nlevels + k, nlevels)
        chunk(at(sib, k), sib).wait_recv()
        chunk(at(sib + other_x - me, k), sib).wait_recv()
        lhs = r.hidden_v[:, pl.ds(pl.multiple_of(z * LEVEL * tall, LEVEL * tall), LEVEL * tall)]
        row = lax.broadcasted_iota(jnp.int32, (tall, LANES), 0)
        col = lax.broadcasted_iota(jnp.int32, (tall, LANES), 1)
        own = (row // rows_dev) == (col // heads)
        tiles = []
        for j in range(LEVEL):
            s = z * LEVEL + j
            dt_w = r.weights[s, tall:tall + rows_dev, :]
            spread = jnp.concatenate([dt_w] * nfsdp, 0)
            tiles.append(jnp.concatenate(
                [r.weights[s, 0:tall, :], jnp.where(own, spread, jnp.zeros_like(spread))], 1))
        res = jnp.dot(lhs, jnp.concatenate(tiles, 0), preferred_element_type=F32)
        r.sums[...] = res if first else r.sums[...] + res

    prev.in_block(1)
    relay(at(me, -1), up, other_x, sib)
    relay(at(me, 1), down, other_x, sib)
    relay(other_x, sib)
    relay(at(me, -2), up, other_x, sib)
    relay(at(me, 2), down, other_x, sib)
    relay(at(other_x, -1), sib)
    relay(at(other_x, 1), sib)
    loads[8].wait()
    level(0, first=True)
    relay(at(me, -3), up, other_x, sib)
    relay(at(me, 3), other_x, sib)
    relay(at(other_x, -2), sib)
    relay(at(other_x, 2), sib)
    level(-1)
    level(1)
    relay(at(me, -4), other_x, sib)
    relay(at(other_x, -3), sib)
    relay(at(other_x, 3), sib)
    level(-2)
    level(2)
    relay(at(other_x, -4), sib)
    prev.scan()
    level(-3)
    level(3)
    level(-4)

    mate = fs + 1 - 2 * part
    r.bc_new[part] = r.sums[:, 0:LANES].astype(BF16)
    swap = pltpu.make_async_remote_copy(
        src_ref=r.bc_new.at[part], dst_ref=r.bc_new.at[part], send_sem=r.swap_send, recv_sem=r.swap_recv,
        device_id={"fsdp": mate}, device_id_type=MESH)
    swap.start()

    def dt_next_of(b, rows):
        v = r.sums[rows, LANES:2 * LANES]
        turn = LANES // 2
        while turn >= heads:
            v = v + pltpu.roll(v, turn, 1)
            turn //= 2
        v = v[:, 0:heads] + r.mine_v[2]
        dt = jnp.maximum(v, 0.0) + jnp.log1p(jnp.exp(-jnp.abs(v)))
        return dt, dt.T

    nxt.factors(dt_next_of)
    nxt.send_keeps()
    loads[7].wait()
    swap.wait_recv()
    nxt.locals()
    nxt.send_locals()
    for b in range(nblocks):
        nxt.in_block(b)
    prev.finish()
    nxt.scan()
    nxt.finish()

    prev.drain()
    nxt.drain()
    swap.wait_send()
    pltpu.make_async_copy(r.weights.at[0, most], r.weights.at[0, most], r.hand_send.at[0]).wait()
    pltpu.make_async_copy(r.dt_rows.at[pl.ds(0, nfsdp - 1)], r.dt_rows.at[pl.ds(0, nfsdp - 1)],
                          r.hand_send.at[1]).wait()
    pltpu.make_async_copy(r.weights.at[pl.ds(0, count - 1)], r.weights.at[pl.ds(0, count - 1)], r.ring_send).wait()


def body(
    hidden_next, values_next, seg_next, proj_bc, proj_dt, dt_bias, decay_rate, skip_gain,
    bc_prev, dt_prev, seg_prev, grad_prev,
):
    tokens, width = values_next.shape
    nfsdp = lax.axis_size("fsdp")
    count = lax.axis_size("seq")
    heads = proj_dt.shape[1] // nfsdp
    head_dim = width // heads
    npair = width // LANES
    nblocks = tokens // SPAN
    share = npair * LANES // count
    rows_dev = proj_bc.shape[0]
    tall = nfsdp * rows_dev

    hbm, vm = (pl.BlockSpec(memory_space=m) for m in (pltpu.HBM, pltpu.VMEM))
    ins = dict(
        seg_next_hbm=(seg_next, hbm), seg_prev_hbm=(seg_prev, hbm),
        proj_bc_hbm=(proj_bc, hbm), proj_dt_hbm=(proj_dt, hbm), dt_prev_hbm=(dt_prev.T, hbm),
        decay_hbm=(decay_rate[None], hbm), skip_hbm=(skip_gain[None], hbm), bias_hbm=(dt_bias[None], hbm),
        hidden_hbm=(hidden_next, hbm), values_hbm=(values_next, hbm), grad_hbm=(grad_prev, hbm),
        bc_prev=(bc_prev, hbm),
    )
    scratch = dict(
        grad_v=pltpu.VMEM((tokens, width), BF16),
        values_v=pltpu.VMEM((tokens, width), BF16),
        hidden_v=pltpu.VMEM(hidden_next.shape, BF16),
        b_prev=pltpu.VMEM((tokens, LANES), BF16),
        c_prev=pltpu.VMEM((tokens, LANES), BF16),
        weights=pltpu.VMEM((count, tall + rows_dev, LANES), BF16),
        dt_rows=pltpu.VMEM((nfsdp, rows_dev, LANES), BF16),
        sums=pltpu.VMEM((tokens, 2 * LANES), F32),
        bc_new=pltpu.VMEM((2, tokens, LANES), BF16),
        proj_bc=pltpu.VMEM(proj_bc.shape, BF16),
        proj_dt=pltpu.VMEM(proj_dt.shape, BF16),
        dt_prev_t=pltpu.VMEM((heads, tokens), F32),
        heads_v=pltpu.VMEM((3, 1, LANES), F32),
        mine_v=pltpu.VMEM((3, 1, heads), F32),
        seg_next=pltpu.SMEM((4,), jnp.int32),
        seg_prev=pltpu.SMEM((4,), jnp.int32),
        load_sem=pltpu.SemaphoreType.DMA((13,)),
        hand_send=pltpu.SemaphoreType.DMA((2,)),
        hand_recv=pltpu.SemaphoreType.DMA((2,)),
        ring_send=pltpu.SemaphoreType.DMA,
        ring_recv=pltpu.SemaphoreType.DMA((count,)),
        swap_send=pltpu.SemaphoreType.DMA,
        swap_recv=pltpu.SemaphoreType.DMA,
    )
    for name in ("prev", "next"):
        for key, val in side_scratch(count, tokens, heads, npair, nblocks, share).items():
            scratch[f"{name}_{key}"] = val
    names = list(ins) + ["out_next", "grad_values"] + list(scratch)
    out = jax.ShapeDtypeStruct((tokens, width), BF16)
    return pl.pallas_call(
        functools.partial(layer_kernel, names, count, nfsdp, (nblocks, heads, head_dim, npair)),
        out_shape=(out, out),
        in_specs=[spec for _, spec in ins.values()],
        out_specs=(vm, vm),
        scratch_shapes=list(scratch.values()),
        compiler_params=pltpu.CompilerParams(
            collective_id=0, has_side_effects=True, vmem_limit_bytes=32 * 1024 * 1024),
        cost_estimate=pl.CostEstimate(flops=4_000_000_000, bytes_accessed=16 * tokens * width, transcendentals=0),
        name="layer",
    )(*[pltpu.with_memory_space_constraint(val, pltpu.HBM) if spec is hbm else val for val, spec in ins.values()])


def solution(mesh):
    in_specs = (
        P("seq", None), P("seq", "fsdp"), P(), P(("seq", "fsdp"), None), P(("seq", "fsdp"), None),
        P(), P(), P(), P("seq", None), P("seq", "fsdp"), P(), P("seq", "fsdp"),
    )
    out_specs = (P("seq", "fsdp"), P("seq", "fsdp"))
    return jax.shard_map(body, mesh=mesh, in_specs=in_specs, out_specs=out_specs, check_vma=False)
```
